32 devices in a mesh: curve: 8 (over z, y), sub: 4 (over x, core).
Axes of the slice: x: 2, y: 2, z: 4, core: 2. Of those that a mesh axis runs over, the one named last changes fastest.
Arguments:
- forcing: float32 [12, 768, 1024], P(None, 'curve', 'sub'), may hold values from -10 to 10
- metric: float32 [768, 1024], P('curve', 'sub'), may hold values from 0.25 to 4
- jacobian: float32 [768, 1024], P('curve', 'sub'), may hold values from 0.5 to 2
- mode_scale: float32 [12], replicated, may hold values from 0.1 to 10
Outputs:
- solution: float32 [12, 768, 1024], P(None, 'curve', 'sub')
- residual: float32 [12, 768, 1024], P(None, 'curve', 'sub')
The draws below stay inside these ranges and needn't reach their ends.
All inputs are finite; a program needn't handle non-finite values.
Results may differ from the reference program's by a relative error of at most 0.0003.
Values sent between devices are 32-bit elements; how exact they have to be, the bound alone decides.
A program may use at most 64 MiB of HBM per device.

```python
import math
import jax
import jax.numpy as jnp
import numpy as np
from jax import lax

NP = 4
MODES = 12
ITERS = 3
EBX = 24
NX = 768
NY = 1024


def draw_forcing(key, part):
    noise_key, scale_key = jax.random.split(jax.random.fold_in(key, 7))
    regions = NX // (NP * EBX)
    region_scale = jnp.exp(jax.random.uniform(scale_key, (regions,), jnp.float32, math.log(0.3), math.log(3.0)))
    per_row = jnp.repeat(region_scale, NP * EBX)
    base = jax.random.normal(noise_key, (MODES, NX, NY), jnp.float32)
    return jnp.clip(base * per_row[None, :, None], -10.0, 10.0)


def block_scale(key, extent, cuts, low, high):
    level, own = 1.0, jax.random.fold_in(key, 6)
    for axis_at, blocks in cuts:
        steps = jnp.exp(jax.random.uniform(jax.random.fold_in(own, axis_at), (blocks,), jnp.float32, low / len(cuts), high / len(cuts)))
        level = level * jnp.repeat(steps, extent[axis_at] // blocks).reshape([-1 if axis == axis_at else 1 for axis in range(len(extent))])
    return level


def setup_inputs(seed: int = 0) -> dict:
    key_list = jax.random.split(jax.random.key(seed), 5)
    forcing = draw_forcing(jax.random.fold_in(key_list[4], 71), 0)
    metric = jnp.clip(jnp.exp(math.log(4.0) - 2.7725887 * jax.random.uniform(key_list[1], (NX, NY), jnp.float32) ** block_scale(key_list[1], (NX, NY), ((0, 8), (1, 4)), -0.2, 0.2)), 0.25, 4.0)
    jacobian = jnp.clip(jnp.exp(math.log(2.0) - 1.3862944 * jax.random.uniform(key_list[2], (NX, NY), jnp.float32) ** block_scale(key_list[2], (NX, NY), ((0, 8), (1, 4)), -0.2, 0.2)), 0.5, 2.0)
    mode_scale = jnp.clip(jnp.exp(jax.random.uniform(key_list[3], (MODES,), jnp.float32, math.log(0.1), math.log(10.0))), 0.1, 10.0)
    return {"forcing": forcing, "metric": metric, "jacobian": jacobian, "mode_scale": mode_scale}


def gll_tables():
    points = np.array([-1.0, -1.0 / math.sqrt(5.0), 1.0 / math.sqrt(5.0), 1.0])
    weights = np.array([1.0 / 6.0, 5.0 / 6.0, 5.0 / 6.0, 1.0 / 6.0])
    factor = np.array([np.prod([points[j] - points[m] for m in range(4) if m != j]) for j in range(4)])
    slopes = np.zeros((4, 4))
    for i in range(4):
        for j in range(4):
            if i != j:
                slopes[i, j] = factor[i] / (factor[j] * (points[i] - points[j]))
        slopes[i, i] = sum((1.0 / (points[i] - points[m]) for m in range(4) if m != i))
    return (slopes, weights)

def line_tables(count):
    phase = jnp.arange(count, dtype=jnp.int32) % 4
    on_edge = (phase == 0) | (phase == 3)
    line_w = jnp.where(on_edge, jnp.float32(1.0 / 6.0), jnp.float32(5.0 / 6.0))
    line_mult = jnp.where(on_edge, jnp.float32(2.0), jnp.float32(1.0))
    return (line_w, line_mult)

def assemble(values):
    for axis_dim in (0, 1):
        phase = lax.broadcasted_iota(jnp.int32, values.shape, axis_dim) % 4
        values = values + jnp.where(phase == 3, jnp.roll(values, -1, axis_dim), 0.0) + jnp.where(phase == 0, jnp.roll(values, 1, axis_dim), 0.0)
    return values

def apply_local(values, scale, slopes, mass_w, flux_w):
    row_count, col_count = values.shape
    shape4 = (row_count // 4, 4, col_count // 4, 4)
    blocks = values.reshape(shape4)
    hp = lax.Precision.HIGHEST
    grad_x = jnp.einsum('ak,xkyb->xayb', slopes, blocks, precision=hp)
    grad_y = jnp.einsum('bk,xayk->xayb', slopes, blocks, precision=hp)
    weight4 = flux_w.reshape(shape4)
    lap = jnp.einsum('ka,xkyb->xayb', slopes, weight4 * grad_x, precision=hp) + jnp.einsum('kb,xayk->xayb', slopes, weight4 * grad_y, precision=hp)
    return mass_w * values + scale * lap.reshape(row_count, col_count)

def diag_terms(flux_w, slopes):
    row_count, col_count = flux_w.shape
    shape4 = (row_count // 4, 4, col_count // 4, 4)
    weight4 = flux_w.reshape(shape4)
    hp = lax.Precision.HIGHEST
    squared = slopes * slopes
    terms = jnp.einsum('ka,xkyb->xayb', squared, weight4, precision=hp) + jnp.einsum('kb,xayk->xayb', squared, weight4, precision=hp)
    return terms.reshape(row_count, col_count)

def reference(forcing, metric, jacobian, mode_scale):
    slopes = jnp.asarray(gll_tables()[0], jnp.float32)
    row_w, row_mult = line_tables(metric.shape[0])
    col_w, col_mult = line_tables(metric.shape[1])
    grid_w = row_w[:, None] * col_w[None, :]
    inv_count = 1.0 / (row_mult[:, None] * col_mult[None, :])
    mass_w = jacobian * grid_w
    flux_w = metric * grid_w
    mass_diag = assemble(mass_w)
    lap_diag = assemble(diag_terms(flux_w, slopes))

    def solve_mode(member):
        source, scale = member
        rhs = assemble(source * mass_w)
        precond = mass_diag + scale * lap_diag
        solution = jnp.zeros_like(rhs)
        residual = rhs
        zvec = residual / precond
        direction = zvec
        rho_now = jnp.sum(residual * zvec * inv_count)
        for iteration in range(ITERS):
            image = assemble(apply_local(direction, scale, slopes, mass_w, flux_w))
            step_len = rho_now / jnp.sum(direction * image * inv_count)
            solution = solution + step_len * direction
            residual = residual - step_len * image
            zvec = residual / precond
            rho_next = jnp.sum(residual * zvec * inv_count)
            direction = zvec + rho_next / rho_now * direction
            rho_now = rho_next
        return (solution, residual)
    solution, residual = lax.map(solve_mode, (forcing, mode_scale))
    return (solution, residual)
```

```python
import functools
import math

import jax
import jax.numpy as jnp
import numpy as np
from jax import lax
from jax.experimental import pallas as pl
from jax.experimental.pallas import tpu as pltpu
from jax.sharding import PartitionSpec as P

ITERS = 3
MESH = pl.DeviceIdType.MESH
LANES = 128
f32 = jnp.float32
bf16 = jnp.bfloat16


def gll_tables():
    points = np.array([-1.0, -1.0 / math.sqrt(5.0), 1.0 / math.sqrt(5.0), 1.0])
    weights = np.array([1.0 / 6.0, 5.0 / 6.0, 5.0 / 6.0, 1.0 / 6.0])
    factor = np.array(
        [np.prod([points[j] - points[m] for m in range(4) if m != j]) for j in range(4)]
    )
    slopes = np.zeros((4, 4))
    for i in range(4):
        for j in range(4):
            if i != j:
                slopes[i, j] = factor[i] / (factor[j] * (points[i] - points[j]))
        slopes[i, i] = sum((1.0 / (points[i] - points[m]) for m in range(4) if m != i))
    return (slopes, weights)


SLOPES, WEIGHTS = gll_tables()


def combo(coefs, parts):
    total = None
    for c, v in zip(coefs, parts):
        if abs(c) < 1e-12:
            continue
        term = v * f32(c)
        total = term if total is None else total + term
    return total


def kernel(
    nc, ns, modes,
    scale_ref, forcing_ref, metric_ref, jac_ref, grad_ref, div_ref,
    sol_ref, res_ref,
    x, r, z, d, s, w, invp, mass, flux, zcat, gout, sums, coef,
    row_tx, row_rx, col_tx, col_rx, cor_rx, ar_tx, ar_rx,
    source, factors, sol_buf, res_buf,
    htx_sem, hrx_sem, atx_sem, arx_sem, in_sem, out_sem,
):
    rows, cols = metric_ref.shape
    tiles = cols // LANES
    loads = []
    for c in range(tiles):
        cut = pl.ds(c * LANES, LANES)
        loads += [
            pltpu.make_async_copy(jac_ref.at[:, cut], factors.at[0, c], in_sem.at[0, c]),
            pltpu.make_async_copy(metric_ref.at[:, cut], factors.at[1, c], in_sem.at[1, c]),
            pltpu.make_async_copy(forcing_ref.at[:, :, cut], source.at[c], in_sem.at[2, c]),
        ]
    for copy in loads:
        copy.start()
    q = rows // 4
    n = nc * ns
    half = cols - LANES
    me_c, me_s = lax.axis_index("curve"), lax.axis_index("sub")
    me = me_c * ns + me_s
    up, down = lax.rem(me_c + nc - 1, nc), lax.rem(me_c + 1, nc)
    left, right = lax.rem(me_s + ns - 1, ns), lax.rem(me_s + 1, ns)

    def place(offset):
        target = lax.rem(me + offset, n)
        return (target // ns, lax.rem(target, ns))

    barrier = pltpu.get_barrier_semaphore()

    def greet(offset, carry):
        pl.semaphore_signal(barrier, inc=1, device_id=place(offset), device_id_type=MESH)
        return carry

    lax.fori_loop(1, n, greet, 0)

    lane_full = lax.broadcasted_iota(jnp.int32, (q, cols), 1)
    lane = lax.broadcasted_iota(jnp.int32, (q, LANES), 1)
    row_at = lax.broadcasted_iota(jnp.int32, (q, cols), 0)
    phase = lane_full % 4
    on_edge = (phase == 0) | (phase == 3)
    take_next = (phase == 3) & (lane_full != cols - 1)
    take_prev = (phase == 0) & (lane_full != 0)
    half_w = [f32(1.0 / 2.0), f32(1.0), f32(1.0), f32(1.0 / 2.0)]

    def load(ref, m):
        return [ref[m, p * q:(p + 1) * q, :] for p in range(4)]

    def save(ref, m, parts):
        for p in range(4):
            ref[m, p * q:(p + 1) * q, :] = parts[p]

    def load2(ref):
        return [ref[p * q:(p + 1) * q, :] for p in range(4)]

    def pack(rd, m, h, tops):
        lo, hi = tops
        row_tx[rd, 0, pl.ds(m, 1), :] = h[0][0:1, :]
        row_tx[rd, 1, pl.ds(m, 1), :] = h[3][q - 1:q, :]
        t0 = h[0] + jnp.where(row_at == 0, 0.0, pltpu.roll(h[3], 1, 0))
        t3 = h[3] + jnp.where(row_at == q - 1, 0.0, pltpu.roll(h[0], q - 1, 0))
        t = [t0, h[1], h[2], t3]
        save(w, m, t)
        for p in range(4):
            at = 4 * m + p
            lo = jnp.where(lane == at, pltpu.roll(t[p][:, :LANES], at, 1), lo)
            hi = jnp.where(lane == at, pltpu.roll(t[p][:, half:], at + 1, 1), hi)
        return lo, hi

    def halo_copies(rd):
        plan = [
            (row_tx.at[rd, 0], row_rx.at[rd, 1], (up, me_s)),
            (row_tx.at[rd, 1], row_rx.at[rd, 0], (down, me_s)),
            (col_tx.at[rd, 0], col_rx.at[rd, 1], (me_c, left)),
            (col_tx.at[rd, 1], col_rx.at[rd, 0], (me_c, right)),
            (col_tx.at[rd, 0, pl.ds(0, 1)], cor_rx.at[rd, 3], (up, left)),
            (col_tx.at[rd, 1, pl.ds(0, 1)], cor_rx.at[rd, 2], (up, right)),
            (col_tx.at[rd, 0, pl.ds(q - 1, 1)], cor_rx.at[rd, 1], (down, left)),
            (col_tx.at[rd, 1, pl.ds(q - 1, 1)], cor_rx.at[rd, 0], (down, right)),
        ]
        return [
            pltpu.make_async_remote_copy(
                src_ref=src, dst_ref=dst, send_sem=htx_sem.at[rd, k], recv_sem=hrx_sem.at[rd, k],
                device_id=where, device_id_type=MESH)
            for k, (src, dst, where) in enumerate(plan)
        ]

    def finish(rd, count):
        for copy in halo_copies(rd):
            copy.wait_recv()
        ph = lax.broadcasted_iota(jnp.int32, (1, LANES), 1) % 4
        edge_row = lax.broadcasted_iota(jnp.int32, (q, LANES), 0)
        merged = []
        for side in range(2):
            above, below = cor_rx[rd, side], cor_rx[rd, 2 + side]
            above = jnp.where(ph == 0, pltpu.roll(above, LANES - 3, 1), 0.0)
            below = jnp.where(ph == 3, pltpu.roll(below, 3, 1), 0.0)
            c = col_rx[rd, side]
            c = c + jnp.where(edge_row == 0, above, 0.0) + jnp.where(edge_row == q - 1, below, 0.0)
            merged.append(c)

        def body(m, carry):
            t = load(w, m)
            t[0] = t[0] + jnp.where(row_at == 0, row_rx[rd, 0, pl.ds(m, 1), :], 0.0)
            t[3] = t[3] + jnp.where(row_at == q - 1, row_rx[rd, 1, pl.ds(m, 1), :], 0.0)
            for p in range(4):
                at = 4 * m + p
                c = t[p] + jnp.where(
                    take_next, pltpu.roll(t[p], cols - 1, 1),
                    jnp.where(take_prev, pltpu.roll(t[p], 1, 1), 0.0))
                a = jnp.where(lane == 0, pltpu.roll(merged[0], LANES - at, 1), 0.0)
                b = jnp.where(lane == LANES - 1, pltpu.roll(merged[1], LANES - 1 - at, 1), 0.0)
                w[m, p * q:(p + 1) * q, :LANES] = c[:, :LANES] + a
                w[m, p * q:(p + 1) * q, half:] = c[:, half:] + b
            return carry

        lax.fori_loop(0, count, body, 0)

    edge_w, mid_w = f32(1.0 / 6.0), f32(5.0 / 6.0)
    col_w = jnp.where(on_edge, edge_w, mid_w)
    mw, fw = [], []
    for copy in loads:
        copy.wait()
    for p in range(4):
        grid_w = col_w * (edge_w if p in (0, 3) else mid_w)
        mw.append(strided([factors.at[0, c] for c in range(tiles)], p, q) * grid_w)
        fw.append(strided([factors.at[1, c] for c in range(tiles)], p, q) * grid_w)
        mass[p * q:(p + 1) * q, :] = mw[p]
        flux[p * q:(p + 1) * q, :] = fw[p]

    zero = jnp.zeros((q, LANES), f32)

    def start_body(m, carry):
        h = [strided([source.at[c, m] for c in range(tiles)], p, q) * mass[p * q:(p + 1) * q, :] for p in range(4)]
        return pack(0, m, h, carry)

    tops = lax.fori_loop(0, modes, start_body, (zero, zero))
    tops = pack(0, modes, mw, tops)
    table = div_ref[:cols, :].astype(f32) + div_ref[2 * cols:, :].astype(f32)
    by_cols = jnp.dot(flux[...], table * table, precision=lax.Precision.HIGHEST,
                      preferred_element_type=f32)
    squared = SLOPES * SLOPES
    lap = [combo(squared[:, a], fw) + by_cols[a * q:(a + 1) * q, :] for a in range(4)]
    lo, hi = pack(0, modes + 1, lap, tops)
    col_tx[0, 0] = lo
    col_tx[0, 1] = hi

    pl.semaphore_wait(barrier, n - 1)
    for copy in halo_copies(0):
        copy.start()
    finish(0, modes + 2)

    def diag_body(m, carry):
        for p in range(4):
            rs = slice(p * q, (p + 1) * q)
            invp[m, rs, :] = 1.0 / (w[modes, rs, :] + scale_ref[m] * w[modes + 1, rs, :])
            r[m, rs, :] = w[m, rs, :]
        return carry

    lax.fori_loop(0, modes, diag_body, 0)

    pad = (lax.broadcasted_iota(jnp.int32, (1, LANES), 1) >= modes).astype(f32)
    eye = lax.broadcasted_iota(jnp.int32, (16, LANES), 0) == lax.broadcasted_iota(
        jnp.int32, (16, LANES), 1)

    def update(it, m):
        a, b = coef[0, pl.ds(m, 1), :], coef[1, pl.ds(m, 1), :]
        zz, ww = load(z, m), load(w, m)
        if it > 1:
            dd, ss = load(d, m), load(s, m)
            zz = [u + b * v for u, v in zip(zz, dd)]
            ww = [u + b * v for u, v in zip(ww, ss)]
            xx = [u + a * v for u, v in zip(load(x, m), zz)]
        else:
            xx = [a * v for v in zz]
        rr = [u - a * v for u, v in zip(load(r, m), ww)]
        return zz, ww, xx, rr

    def fill(m, parts):
        v = jnp.concatenate(parts, axis=0)
        top = v.astype(bf16)
        at = pl.ds(pl.multiple_of(m * rows, rows), rows)
        zcat[at, :cols] = top
        zcat[at, cols:] = (v - top.astype(f32)).astype(bf16)

    def multiply(table_ref):
        gout[...] = (
            jnp.dot(zcat[...], table_ref[:2 * cols, :], preferred_element_type=f32)
            + jnp.dot(zcat[:, :cols], table_ref[2 * cols:, :], preferred_element_type=f32))

    rho_old = step_old = None
    for it in range(ITERS):
        rd = it + 1

        def first(m, carry, it=it):
            if it == 0:
                rr = load(r, m)
            else:
                dd, ss, xx, rr = update(it, m)
                save(r, m, rr)
                save(x, m, xx)
                save(d, m, dd)
                save(s, m, ss)
            zz = [u * v for u, v in zip(rr, load(invp, m))]
            save(z, m, zz)
            fill(m, zz)
            rz = [u * v for u, v in zip(rr, zz)]
            rho = (rz[0] + rz[3]) * 0.5 + (rz[1] + rz[2])
            rho = jnp.where(on_edge, rho * 0.5, rho)
            sums[0, pl.ds(m, 1), :] = jnp.sum(rho, axis=0, keepdims=True)
            f = load2(flux)
            fg = [f[a] * combo(SLOPES[a], zz) * scale_ref[m] for a in range(4)]
            ms = load2(mass)
            save(w, m, [ms[a] * zz[a] + combo(SLOPES[:, a], fg) for a in range(4)])
            return carry

        lax.fori_loop(0, modes, first, 0)
        multiply(grad_ref)

        def second(m, carry):
            g = gout[pl.ds(pl.multiple_of(m * rows, rows), rows), :]
            fg = flux[...] * g * scale_ref[m]
            fill(m, [fg])
            return carry

        lax.fori_loop(0, modes, second, 0)
        multiply(div_ref)

        def third(m, carry, rd=rd):
            zz = load(z, m)
            h = [u + gout[pl.ds(pl.multiple_of(m * rows + p * q, q), q), :]
                 for p, u in enumerate(load(w, m))]
            zh = zz[0] * h[0] + zz[1] * h[1] + zz[2] * h[2] + zz[3] * h[3]
            sums[1, pl.ds(m, 1), :] = jnp.sum(zh, axis=0, keepdims=True)
            return pack(rd, m, h, carry)

        lo, hi = lax.fori_loop(0, modes, third, (zero, zero))
        col_tx[rd, 0] = lo
        col_tx[rd, 1] = hi
        for k in range(2):
            part = jnp.sum(sums[k], axis=1, keepdims=True)
            line = jnp.sum(jnp.where(eye, part, 0.0), axis=0, keepdims=True)
            ar_tx[it, k:k + 1, :] = line
            ar_rx[it, 0, k:k + 1, :] = line
        for copy in halo_copies(rd):
            copy.start()

        def spread(offset, carry, it=it):
            pltpu.make_async_remote_copy(
                src_ref=ar_tx.at[it], dst_ref=ar_rx.at[it, offset],
                send_sem=atx_sem.at[it], recv_sem=arx_sem.at[it],
                device_id=place(offset), device_id_type=MESH).start()
            return carry

        lax.fori_loop(1, n, spread, 0)
        finish(rd, modes)
        gathered = ar_rx.at[it, pl.ds(1, n - 1)]
        pltpu.make_async_copy(gathered, gathered, arx_sem.at[it]).wait()
        total = jnp.sum(ar_rx[it], axis=0)
        rho, curve_sum = total[0:1] + pad, total[1:2] + pad
        if it == 0:
            mixing = jnp.zeros_like(rho)
            step_len = rho / curve_sum
        else:
            mixing = rho / rho_old
            step_len = rho / (curve_sum - mixing * rho / step_old)
        for k, line in enumerate((step_len, mixing)):
            tall = jnp.sum(jnp.where(eye, line, 0.0), axis=1, keepdims=True)
            coef[k] = jnp.broadcast_to(tall, (16, cols))
        rho_old, step_old = rho, step_len

    def stores(m):
        return [
            pltpu.make_async_copy(
                buf.at[c, m], out.at[m, :, pl.ds(c * LANES, LANES)], out_sem.at[k, c, m])
            for k, (buf, out) in enumerate(((sol_buf, sol_ref), (res_buf, res_ref)))
            for c in range(tiles)
        ]

    def last(m, carry):
        _, _, xx, rr = update(ITERS, m)
        for c in range(tiles):
            for p in range(4):
                cut = slice(c * LANES, (c + 1) * LANES)
                sol_buf[c, m, pl.ds(p, q, stride=4), :] = xx[p][:, cut]
                res_buf[c, m, pl.ds(p, q, stride=4), :] = rr[p][:, cut]
        for copy in stores(m):
            copy.start()
        return carry

    lax.fori_loop(0, modes, last, 0)

    for rd in range(ITERS + 1):
        for copy in halo_copies(rd):
            copy.wait_send()
    for it in range(ITERS):
        sent = ar_rx.at[it, pl.ds(1, n - 1)]
        pltpu.make_async_copy(sent, sent, atx_sem.at[it]).wait()

    def drain(m, carry):
        for copy in stores(m):
            copy.wait()
        return carry

    lax.fori_loop(0, modes, drain, 0)


def strided(refs, p, q):
    return jnp.concatenate([ref[pl.ds(p, q, stride=4), :] for ref in refs], axis=1)


def stack_table(table):
    top = table.astype(bf16)
    low = (table - top.astype(np.float32)).astype(bf16)
    return np.concatenate([top, top, low], axis=0)


def shards(nc, ns, forcing, metric, jacobian, mode_scale):
    modes, rows, cols = forcing.shape
    block = np.kron(np.eye(cols // 4), SLOPES).astype(np.float32)
    grad, div = stack_table(block.T), stack_table(block)
    n, q = nc * ns, rows // 4
    vm = pl.BlockSpec(memory_space=pltpu.VMEM)
    hbm = pl.BlockSpec(memory_space=pl.ANY)
    rounds = ITERS + 1
    tiles = cols // LANES
    split = pltpu.VMEM((tiles, modes, rows, LANES), f32)
    field = pltpu.VMEM((modes, rows, cols), f32)
    return pl.pallas_call(
        functools.partial(kernel, nc, ns, modes),
        out_shape=[jax.ShapeDtypeStruct(forcing.shape, f32)] * 2,
        in_specs=[pl.BlockSpec(memory_space=pltpu.SMEM)] + [hbm] * 3 + [vm] * 2,
        out_specs=[hbm, hbm],
        scratch_shapes=[
            field, field, field, field, field,
            pltpu.VMEM((modes + 2, rows, cols), f32),
            field,
            pltpu.VMEM((rows, cols), f32),
            pltpu.VMEM((rows, cols), f32),
            pltpu.VMEM((modes * rows, 2 * cols), bf16),
            pltpu.VMEM((modes * rows, cols), f32),
            pltpu.VMEM((2, 16, cols), f32),
            pltpu.VMEM((2, 16, cols), f32),
            pltpu.VMEM((rounds, 2, 16, cols), f32),
            pltpu.VMEM((rounds, 2, 16, cols), f32),
            pltpu.VMEM((rounds, 2, q, LANES), f32),
            pltpu.VMEM((rounds, 2, q, LANES), f32),
            pltpu.VMEM((rounds, 4, 1, LANES), f32),
            pltpu.VMEM((ITERS, 2, LANES), f32),
            pltpu.VMEM((ITERS, n, 2, LANES), f32),
            split,
            pltpu.VMEM((2, tiles, rows, LANES), f32),
            split, split,
            pltpu.SemaphoreType.DMA((rounds, 8)),
            pltpu.SemaphoreType.DMA((rounds, 8)),
            pltpu.SemaphoreType.DMA((ITERS,)),
            pltpu.SemaphoreType.DMA((ITERS,)),
            pltpu.SemaphoreType.DMA((3, tiles)),
            pltpu.SemaphoreType.DMA((2, tiles, modes)),
        ],
        compiler_params=pltpu.CompilerParams(
            collective_id=0, has_side_effects=True, vmem_limit_bytes=48 * 1024 * 1024),
    )(mode_scale, forcing, metric, jacobian, jnp.asarray(grad), jnp.asarray(div))


def solution(mesh):
    placed = (P(None, "curve", "sub"), P("curve", "sub"), P("curve", "sub"), P())
    return jax.shard_map(
        functools.partial(shards, mesh.shape["curve"], mesh.shape["sub"]),
        mesh=mesh,
        in_specs=placed,
        out_specs=(P(None, "curve", "sub"), P(None, "curve", "sub")),
        check_vma=False,
    )
```

```python
import functools
import math

import jax
import jax.numpy as jnp
import numpy as np
from jax import lax
from jax.experimental import pallas as pl
from jax.experimental.pallas import tpu as pltpu
from jax.sharding import PartitionSpec as P

ITERS = 3
GROUPS = 2
UNROLL = 2
MESH = pl.DeviceIdType.MESH
LANES = 128
f32 = jnp.float32
bf16 = jnp.bfloat16


def gll_tables():
    points = np.array([-1.0, -1.0 / math.sqrt(5.0), 1.0 / math.sqrt(5.0), 1.0])
    weights = np.array([1.0 / 6.0, 5.0 / 6.0, 5.0 / 6.0, 1.0 / 6.0])
    factor = np.array(
        [np.prod([points[j] - points[m] for m in range(4) if m != j]) for j in range(4)]
    )
    slopes = np.zeros((4, 4))
    for i in range(4):
        for j in range(4):
            if i != j:
                slopes[i, j] = factor[i] / (factor[j] * (points[i] - points[j]))
        slopes[i, i] = sum((1.0 / (points[i] - points[m]) for m in range(4) if m != i))
    return (slopes, weights)


SLOPES, WEIGHTS = gll_tables()


def combo(coefs, parts):
    total = None
    for c, v in zip(coefs, parts):
        if abs(c) < 1e-12:
            continue
        term = v * f32(c)
        total = term if total is None else total + term
    return total


def kernel(
    nc, ns, modes, groups,
    scale_hbm, forcing_ref, metric_ref, jac_ref, grad_hbm, div_hbm,
    x, r,
    z, d, s, w, invp, mass, flux, zcat, gout, sums, coef,
    row_tx, row_rx, col_tx, col_rx, cor_rx, ar_tx, ar_rx,
    source, factors, grad_ref, div_ref, scale_ref,
    htx_sem, hrx_sem, atx_sem, arx_sem, in_sem, table_sem,
):
    rows, cols = metric_ref.shape
    q = rows // 4
    n = nc * ns
    half = cols - LANES
    tiles = cols // LANES
    per = modes // groups
    slots = row_tx.shape[2]
    loads, sources = [], []
    for c in range(tiles):
        cut = pl.ds(c * LANES, LANES)
        loads += [
            pltpu.make_async_copy(jac_ref.at[:, cut], factors.at[0, c], in_sem.at[0, c]),
            pltpu.make_async_copy(metric_ref.at[:, cut], factors.at[1, c], in_sem.at[1, c]),
        ]
        sources.append(
            pltpu.make_async_copy(forcing_ref.at[:, :, cut], source.at[c], in_sem.at[2, c]))
    div_load = pltpu.make_async_copy(div_hbm, div_ref, table_sem.at[0])
    grad_load = pltpu.make_async_copy(grad_hbm, grad_ref, table_sem.at[1])
    scale_load = pltpu.make_async_copy(scale_hbm, scale_ref, table_sem.at[2])
    for copy in loads + sources + [div_load, scale_load, grad_load]:
        copy.start()

    me_c, me_s = lax.axis_index("curve"), lax.axis_index("sub")
    me = me_c * ns + me_s
    up, down = lax.rem(me_c + nc - 1, nc), lax.rem(me_c + 1, nc)
    left, right = lax.rem(me_s + ns - 1, ns), lax.rem(me_s + 1, ns)

    def place(offset):
        target = lax.rem(me + offset, n)
        return (target // ns, lax.rem(target, ns))

    barrier = pltpu.get_barrier_semaphore()

    def greet(offset, carry):
        pl.semaphore_signal(barrier, inc=1, device_id=place(offset), device_id_type=MESH)
        return carry

    lax.fori_loop(1, n, greet, 0)

    lane_full = lax.broadcasted_iota(jnp.int32, (q, cols), 1)
    lane = lax.broadcasted_iota(jnp.int32, (q, LANES), 1)
    row_at = lax.broadcasted_iota(jnp.int32, (q, cols), 0)
    phase = lane_full % 4
    on_edge = (phase == 0) | (phase == 3)
    take_next = (phase == 3) & (lane_full != cols - 1)
    take_prev = (phase == 0) & (lane_full != 0)

    def load(ref, m):
        return [ref[m, p * q:(p + 1) * q, :] for p in range(4)]

    def save(ref, m, parts):
        for p in range(4):
            ref[m, p * q:(p + 1) * q, :] = parts[p]

    def load2(ref):
        return [ref[p * q:(p + 1) * q, :] for p in range(4)]

    def pack(k, m, slot, h, tops):
        lo, hi = tops
        row_tx[k, 0, pl.ds(slot, 1), :] = h[0][0:1, :]
        row_tx[k, 1, pl.ds(slot, 1), :] = h[3][q - 1:q, :]
        t0 = h[0] + jnp.where(row_at == 0, 0.0, pltpu.roll(h[3], 1, 0))
        t3 = h[3] + jnp.where(row_at == q - 1, 0.0, pltpu.roll(h[0], q - 1, 0))
        t = [t0, h[1], h[2], t3]
        save(w, m, t)
        for p in range(4):
            at = 4 * slot + p
            lo = jnp.where(lane == at, pltpu.roll(t[p][:, :LANES], at, 1), lo)
            hi = jnp.where(lane == at, pltpu.roll(t[p][:, half:], at + 1, 1), hi)
        return lo, hi

    def halo_copies(k):
        plan = [
            (col_tx.at[k, 0, pl.ds(0, 1)], cor_rx.at[k, 3], (up, left)),
            (col_tx.at[k, 1, pl.ds(0, 1)], cor_rx.at[k, 2], (up, right)),
            (col_tx.at[k, 0, pl.ds(q - 1, 1)], cor_rx.at[k, 1], (down, left)),
            (col_tx.at[k, 1, pl.ds(q - 1, 1)], cor_rx.at[k, 0], (down, right)),
            (row_tx.at[k, 0], row_rx.at[k, 1], (up, me_s)),
            (row_tx.at[k, 1], row_rx.at[k, 0], (down, me_s)),
            (col_tx.at[k, 0], col_rx.at[k, 1], (me_c, left)),
            (col_tx.at[k, 1], col_rx.at[k, 0], (me_c, right)),
        ]
        return [
            pltpu.make_async_remote_copy(
                src_ref=src, dst_ref=dst, send_sem=htx_sem.at[k, e], recv_sem=hrx_sem.at[k, e],
                device_id=where, device_id_type=MESH)
            for e, (src, dst, where) in enumerate(plan)
        ]

    def send(k, tops):
        col_tx[k, 0], col_tx[k, 1] = tops
        for copy in halo_copies(k):
            copy.start()

    def arrive(k):
        for copy in halo_copies(k):
            copy.wait_recv()
        ph = lax.broadcasted_iota(jnp.int32, (1, LANES), 1) % 4
        edge_row = lax.broadcasted_iota(jnp.int32, (q, LANES), 0)
        merged = []
        for side in range(2):
            above, below = cor_rx[k, side], cor_rx[k, 2 + side]
            above = jnp.where(ph == 0, pltpu.roll(above, LANES - 3, 1), 0.0)
            below = jnp.where(ph == 3, pltpu.roll(below, 3, 1), 0.0)
            c = col_rx[k, side]
            c = c + jnp.where(edge_row == 0, above, 0.0) + jnp.where(edge_row == q - 1, below, 0.0)
            merged.append(c)
        return merged

    def assembled(k, m, slot, merged):
        t = load(w, m)
        t[0] = t[0] + jnp.where(row_at == 0, row_rx[k, 0, pl.ds(slot, 1), :], 0.0)
        t[3] = t[3] + jnp.where(row_at == q - 1, row_rx[k, 1, pl.ds(slot, 1), :], 0.0)
        out = []
        for p in range(4):
            at = 4 * slot + p
            c = t[p] + jnp.where(
                take_next, pltpu.roll(t[p], cols - 1, 1),
                jnp.where(take_prev, pltpu.roll(t[p], 1, 1), 0.0))
            a = jnp.where(lane == 0, pltpu.roll(merged[0], LANES - at, 1), 0.0)
            b = jnp.where(lane == LANES - 1, pltpu.roll(merged[1], LANES - 1 - at, 1), 0.0)
            pieces = [c[:, e * LANES:(e + 1) * LANES] for e in range(tiles)]
            pieces[0] = pieces[0] + a
            pieces[-1] = pieces[-1] + b
            out.append(jnp.concatenate(pieces, axis=1))
        return out

    edge_w, mid_w = f32(1.0 / 6.0), f32(5.0 / 6.0)
    col_w = jnp.where(on_edge, edge_w, mid_w)
    mw, fw = [], []
    for copy in loads:
        copy.wait()
    for p in range(4):
        grid_w = col_w * (edge_w if p in (0, 3) else mid_w)
        mw.append(strided([factors.at[0, c] for c in range(tiles)], p, q) * grid_w)
        fw.append(strided([factors.at[1, c] for c in range(tiles)], p, q) * grid_w)
        mass[p * q:(p + 1) * q, :] = mw[p]
        flux[p * q:(p + 1) * q, :] = fw[p]
    zero = jnp.zeros((q, LANES), f32)
    tops = pack(0, modes, per, mw, (zero, zero))
    div_load.wait()
    table = div_ref[:cols, :].astype(f32) + div_ref[2 * cols:, :].astype(f32)
    by_cols = jnp.dot(flux[...], table * table, precision=lax.Precision.HIGHEST,
                      preferred_element_type=f32)
    squared = SLOPES * SLOPES
    lap = [combo(squared[:, a], fw) + by_cols[a * q:(a + 1) * q, :] for a in range(4)]
    tops = pack(0, modes + 1, per + 1, lap, tops)
    for copy in sources:
        copy.wait()
    for g in range(groups):

        def start_body(slot, carry, g=g):
            m = g * per + slot
            h = [strided([source.at[c, m] for c in range(tiles)], p, q)
                 * mass[p * q:(p + 1) * q, :] for p in range(4)]
            return pack(g, m, slot, h, carry)

        tops = lax.fori_loop(0, per, start_body, tops if g == 0 else (zero, zero), unroll=UNROLL)
        if g == 0:
            pl.semaphore_wait(barrier, n - 1)
        send(g, tops)
    scale_load.wait()
    grad_load.wait()

    pad = (lax.broadcasted_iota(jnp.int32, (1, LANES), 1) >= per).astype(f32)
    eye = lax.broadcasted_iota(jnp.int32, (slots, LANES), 0) == lax.broadcasted_iota(
        jnp.int32, (slots, LANES), 1)

    def update(it, g, m, slot, ww):
        a, b = coef[g, 0, pl.ds(slot, 1), :], coef[g, 1, pl.ds(slot, 1), :]
        zz = load(z, m)
        if it > 1:
            dd, ss = load(d, m), load(s, m)
            zz = [u + b * v for u, v in zip(zz, dd)]
            ww = [u + b * v for u, v in zip(ww, ss)]
            xx = [u + a * v for u, v in zip(load(x, m), zz)]
        else:
            xx = [a * v for v in zz]
        rr = [u - a * v for u, v in zip(load(r, m), ww)]
        return zz, ww, xx, rr

    def fill(slot, parts):
        v = jnp.concatenate(parts, axis=0)
        top = v.astype(bf16)
        at = pl.ds(pl.multiple_of(slot * rows, rows), rows)
        zcat[at, :cols] = top
        zcat[at, cols:] = (v - top.astype(f32)).astype(bf16)

    def multiply(table_ref):
        gout[...] = (
            jnp.dot(zcat[...], table_ref[:2 * cols, :], preferred_element_type=f32)
            + jnp.dot(zcat[:, :cols], table_ref[2 * cols:, :], preferred_element_type=f32))

    old = [None] * groups

    def coefficients(it, g):
        k = it * groups + g
        gathered = ar_rx.at[k, pl.ds(1, n - 1)]
        pltpu.make_async_copy(gathered, gathered, arx_sem.at[k]).wait()
        total = jnp.sum(ar_rx[k], axis=0)
        rho, curve_sum = total[0:1] + pad, total[1:2] + pad
        if it == 0:
            mixing = jnp.zeros_like(rho)
            step_len = rho / curve_sum
        else:
            mixing = rho / old[g][0]
            step_len = rho / (curve_sum - mixing * rho / old[g][1])
        for e, line in enumerate((step_len, mixing)):
            tall = jnp.sum(jnp.where(eye, line, 0.0), axis=1, keepdims=True)
            coef[g, e] = jnp.broadcast_to(tall, (slots, cols))
        old[g] = (rho, step_len)

    for it in range(ITERS):
        for g in range(groups):
            base = g * per
            k = it * groups + g
            merged = arrive(k)
            if it == 0 and g == 0:
                for e in range(2):
                    save(w, modes + e, assembled(k, modes + e, per + e, merged))
            if it > 0:
                coefficients(it - 1, g)

            def first(slot, carry, it=it, g=g, k=k, base=base, merged=merged):
                m = base + slot
                ww = assembled(k, m, slot, merged)
                if it == 0:
                    rr = ww
                    inv = [1.0 / (u + scale_ref[m] * v)
                           for u, v in zip(load(w, modes), load(w, modes + 1))]
                    save(invp, m, inv)
                else:
                    dd, ss, xx, rr = update(it, g, m, slot, ww)
                    save(x, m, xx)
                    save(d, m, dd)
                    save(s, m, ss)
                    inv = load(invp, m)
                save(r, m, rr)
                zz = [u * v for u, v in zip(rr, inv)]
                save(z, m, zz)
                fill(slot, zz)
                rz = [u * v for u, v in zip(rr, zz)]
                rho = (rz[0] + rz[3]) * 0.5 + (rz[1] + rz[2])
                rho = jnp.where(on_edge, rho * 0.5, rho)
                sums[0, pl.ds(slot, 1), :] = jnp.sum(rho, axis=0, keepdims=True)
                f = load2(flux)
                fg = [f[a] * combo(SLOPES[a], zz) * scale_ref[m] for a in range(4)]
                ms = load2(mass)
                save(w, m, [ms[a] * zz[a] + combo(SLOPES[:, a], fg) for a in range(4)])
                return carry

            lax.fori_loop(0, per, first, 0, unroll=UNROLL)
            multiply(grad_ref)

            def second(slot, carry, base=base):
                grad = gout[pl.ds(pl.multiple_of(slot * rows, rows), rows), :]
                fill(slot, [flux[...] * grad * scale_ref[base + slot]])
                return carry

            lax.fori_loop(0, per, second, 0, unroll=UNROLL)
            multiply(div_ref)

            def third(slot, carry, k=k, base=base):
                m = base + slot
                zz = load(z, m)
                h = [u + gout[pl.ds(pl.multiple_of(slot * rows + p * q, q), q), :]
                     for p, u in enumerate(load(w, m))]
                zh = zz[0] * h[0] + zz[1] * h[1] + zz[2] * h[2] + zz[3] * h[3]
                sums[1, pl.ds(slot, 1), :] = jnp.sum(zh, axis=0, keepdims=True)
                return pack(k + groups, m, slot, h, carry)

            tops = lax.fori_loop(0, per, third, (zero, zero), unroll=UNROLL)
            send(k + groups, tops)
            for e in range(2):
                part = jnp.sum(sums[e], axis=1, keepdims=True)
                line = jnp.sum(jnp.where(eye, part, 0.0), axis=0, keepdims=True)
                ar_tx[k, e:e + 1, :] = line
                ar_rx[k, 0, e:e + 1, :] = line

            def spread(offset, carry, k=k):
                pltpu.make_async_remote_copy(
                    src_ref=ar_tx.at[k], dst_ref=ar_rx.at[k, offset],
                    send_sem=atx_sem.at[k], recv_sem=arx_sem.at[k],
                    device_id=place(offset), device_id_type=MESH).start()
                return carry

            lax.fori_loop(1, n, spread, 0)

    for g in range(groups):
        k = ITERS * groups + g
        merged = arrive(k)
        coefficients(ITERS - 1, g)

        def last(slot, carry, g=g, k=k, merged=merged):
            m = g * per + slot
            _, _, xx, rr = update(ITERS, g, m, slot, assembled(k, m, slot, merged))
            save(x, m, xx)
            save(r, m, rr)
            return carry

        lax.fori_loop(0, per, last, 0, unroll=UNROLL)

    for k in range((ITERS + 1) * groups):
        for copy in halo_copies(k):
            copy.wait_send()
    for k in range(ITERS * groups):
        sent = ar_rx.at[k, pl.ds(1, n - 1)]
        pltpu.make_async_copy(sent, sent, atx_sem.at[k]).wait()


def node_order(x, r, sol_ref, res_ref, sol_buf, res_buf, sem):
    modes, rows, cols = x.shape
    q, tiles = rows // 4, cols // LANES

    def stores(m):
        return [
            pltpu.make_async_copy(
                buf.at[c, m], out.at[m, :, pl.ds(c * LANES, LANES)], sem.at[k, c, m])
            for k, (buf, out) in enumerate(((sol_buf, sol_ref), (res_buf, res_ref)))
            for c in range(tiles)
        ]

    def body(m, carry):
        for c in range(tiles):
            for p in range(4):
                cut = slice(c * LANES, (c + 1) * LANES)
                sol_buf[c, m, pl.ds(p, q, stride=4), :] = x[m, p * q:(p + 1) * q, cut]
                res_buf[c, m, pl.ds(p, q, stride=4), :] = r[m, p * q:(p + 1) * q, cut]
        for copy in stores(m):
            copy.start()
        return carry

    lax.fori_loop(0, modes, body, 0)

    def drain(m, carry):
        for copy in stores(m):
            copy.wait()
        return carry

    lax.fori_loop(0, modes, drain, 0)


def strided(refs, p, q):
    return jnp.concatenate([ref[pl.ds(p, q, stride=4), :] for ref in refs], axis=1)


def stack_table(table):
    top = table.astype(bf16)
    low = (table - top.astype(np.float32)).astype(bf16)
    return np.concatenate([top, top, low], axis=0)


def shards(nc, ns, forcing, metric, jacobian, mode_scale):
    modes, rows, cols = forcing.shape
    block = np.kron(np.eye(cols // 4), SLOPES).astype(np.float32)
    grad, div = stack_table(block.T), stack_table(block)
    n, q, tiles = nc * ns, rows // 4, cols // LANES
    groups = GROUPS if modes % GROUPS == 0 else 1
    per = modes // groups
    slots = -(-(per + 2) // 8) * 8
    vm = pl.BlockSpec(memory_space=pltpu.VMEM)
    hbm = pl.BlockSpec(memory_space=pltpu.HBM)
    rounds, sums = (ITERS + 1) * groups, ITERS * groups
    field = pltpu.VMEM((modes, rows, cols), f32)
    split = pltpu.VMEM((tiles, modes, rows, LANES), f32)
    table = pltpu.VMEM(grad.shape, bf16)
    shape = jax.ShapeDtypeStruct(forcing.shape, f32)
    x, r = pl.pallas_call(
        functools.partial(kernel, nc, ns, modes, groups),
        out_shape=[shape] * 2,
        in_specs=[hbm] * 6,
        out_specs=[vm, vm],
        scratch_shapes=[
            field, field, field,
            pltpu.VMEM((modes + 2, rows, cols), f32),
            field,
            pltpu.VMEM((rows, cols), f32),
            pltpu.VMEM((rows, cols), f32),
            pltpu.VMEM((per * rows, 2 * cols), bf16),
            pltpu.VMEM((per * rows, cols), f32),
            pltpu.VMEM((2, slots, cols), f32),
            pltpu.VMEM((groups, 2, slots, cols), f32),
            pltpu.VMEM((rounds, 2, slots, cols), f32),
            pltpu.VMEM((rounds, 2, slots, cols), f32),
            pltpu.VMEM((rounds, 2, q, LANES), f32),
            pltpu.VMEM((rounds, 2, q, LANES), f32),
            pltpu.VMEM((rounds, 4, 1, LANES), f32),
            pltpu.VMEM((sums, 2, LANES), f32),
            pltpu.VMEM((sums, n, 2, LANES), f32),
            split,
            pltpu.VMEM((2, tiles, rows, LANES), f32),
            table, table,
            pltpu.SMEM((modes,), f32),
            pltpu.SemaphoreType.DMA((rounds, 8)),
            pltpu.SemaphoreType.DMA((rounds, 8)),
            pltpu.SemaphoreType.DMA((sums,)),
            pltpu.SemaphoreType.DMA((sums,)),
            pltpu.SemaphoreType.DMA((3, tiles)),
            pltpu.SemaphoreType.DMA((3,)),
        ],
        compiler_params=pltpu.CompilerParams(
            collective_id=0, has_side_effects=True, vmem_limit_bytes=63000000),
    )(mode_scale, forcing, metric, jacobian, jnp.asarray(grad), jnp.asarray(div))
    return pl.pallas_call(
        node_order,
        out_shape=[shape] * 2,
        in_specs=[vm, vm],
        out_specs=[hbm, hbm],
        scratch_shapes=[split, split, pltpu.SemaphoreType.DMA((2, tiles, modes))],
        compiler_params=pltpu.CompilerParams(vmem_limit_bytes=16 * 1024 * 1024),
    )(x, r)


def solution(mesh):
    placed = (P(None, "curve", "sub"), P("curve", "sub"), P("curve", "sub"), P())
    return jax.shard_map(
        functools.partial(shards, mesh.shape["curve"], mesh.shape["sub"]),
        mesh=mesh,
        in_specs=placed,
        out_specs=(P(None, "curve", "sub"), P(None, "curve", "sub")),
        check_vma=False,
    )
```

```python
import functools
import math

import jax
import jax.numpy as jnp
import numpy as np
from jax import lax
from jax.experimental import pallas as pl
from jax.experimental.pallas import tpu as pltpu
from jax.sharding import PartitionSpec as P

ITERS = 3
GROUPS = 2
UNROLL = True
MESH = pl.DeviceIdType.MESH
LANES = 128
f32 = jnp.float32
bf16 = jnp.bfloat16


def gll_tables():
    points = np.array([-1.0, -1.0 / math.sqrt(5.0), 1.0 / math.sqrt(5.0), 1.0])
    weights = np.array([1.0 / 6.0, 5.0 / 6.0, 5.0 / 6.0, 1.0 / 6.0])
    factor = np.array(
        [np.prod([points[j] - points[m] for m in range(4) if m != j]) for j in range(4)]
    )
    slopes = np.zeros((4, 4))
    for i in range(4):
        for j in range(4):
            if i != j:
                slopes[i, j] = factor[i] / (factor[j] * (points[i] - points[j]))
        slopes[i, i] = sum((1.0 / (points[i] - points[m]) for m in range(4) if m != i))
    return (slopes, weights)


SLOPES, WEIGHTS = gll_tables()


def combo(coefs, parts):
    total = None
    for c, v in zip(coefs, parts):
        if abs(c) < 1e-12:
            continue
        term = v * f32(c)
        total = term if total is None else total + term
    return total


def kernel(
    nc, ns, modes, groups,
    scale_hbm, forcing_ref, metric_ref, jac_ref, grad_hbm, div_hbm,
    x, r,
    z, d, s, w, invp, mass, flux, zcat, gout, sums, coef,
    row_tx, row_rx, col_tx, col_rx, cor_rx, ar_tx, ar_rx,
    source, factors, grad_ref, div_ref, scale_ref,
    htx_sem, hrx_sem, atx_sem, arx_sem, in_sem, table_sem,
):
    rows, cols = metric_ref.shape
    q = rows // 4
    n = nc * ns
    half = cols - LANES
    tiles = cols // LANES
    per = modes // groups
    slots = row_tx.shape[2]
    loads, sources = [], []
    for c in range(tiles):
        cut = pl.ds(c * LANES, LANES)
        loads += [
            pltpu.make_async_copy(jac_ref.at[:, cut], factors.at[0, c], in_sem.at[0, c]),
            pltpu.make_async_copy(metric_ref.at[:, cut], factors.at[1, c], in_sem.at[1, c]),
        ]
        sources.append(
            pltpu.make_async_copy(forcing_ref.at[:, :, cut], source.at[c], in_sem.at[2, c]))
    div_load = pltpu.make_async_copy(div_hbm, div_ref, table_sem.at[0])
    grad_load = pltpu.make_async_copy(grad_hbm, grad_ref, table_sem.at[1])
    scale_load = pltpu.make_async_copy(scale_hbm, scale_ref, table_sem.at[2])
    for copy in loads + sources + [div_load, scale_load, grad_load]:
        copy.start()

    me_c, me_s = lax.axis_index("curve"), lax.axis_index("sub")
    me = me_c * ns + me_s
    up, down = lax.rem(me_c + nc - 1, nc), lax.rem(me_c + 1, nc)
    left, right = lax.rem(me_s + ns - 1, ns), lax.rem(me_s + 1, ns)

    def place(offset):
        target = lax.rem(me + offset, n)
        return (target // ns, lax.rem(target, ns))

    barrier = pltpu.get_barrier_semaphore()

    def greet(offset, carry):
        pl.semaphore_signal(barrier, inc=1, device_id=place(offset), device_id_type=MESH)
        return carry

    lax.fori_loop(1, n, greet, 0)

    lane_full = lax.broadcasted_iota(jnp.int32, (q, cols), 1)
    lane = lax.broadcasted_iota(jnp.int32, (q, LANES), 1)
    row_at = lax.broadcasted_iota(jnp.int32, (q, cols), 0)
    phase = lane_full % 4
    on_edge = (phase == 0) | (phase == 3)
    take_next = (phase == 3) & (lane_full != cols - 1)
    take_prev = (phase == 0) & (lane_full != 0)

    def load(ref, m):
        return [ref[m, p * q:(p + 1) * q, :] for p in range(4)]

    def save(ref, m, parts):
        for p in range(4):
            ref[m, p * q:(p + 1) * q, :] = parts[p]

    def load2(ref):
        return [ref[p * q:(p + 1) * q, :] for p in range(4)]

    def pack(k, m, slot, h, tops):
        lo, hi = tops
        row_tx[k, 0, pl.ds(slot, 1), :] = h[0][0:1, :]
        row_tx[k, 1, pl.ds(slot, 1), :] = h[3][q - 1:q, :]
        t0 = h[0] + jnp.where(row_at == 0, 0.0, pltpu.roll(h[3], 1, 0))
        t3 = h[3] + jnp.where(row_at == q - 1, 0.0, pltpu.roll(h[0], q - 1, 0))
        t = [t0, h[1], h[2], t3]
        save(w, m, t)
        for p in range(4):
            at = 4 * slot + p
            lo = jnp.where(lane == at, pltpu.roll(t[p][:, :LANES], at, 1), lo)
            hi = jnp.where(lane == at, pltpu.roll(t[p][:, half:], at + 1, 1), hi)
        return lo, hi

    def halo_copies(k):
        plan = [
            (col_tx.at[k, 0, pl.ds(0, 1)], cor_rx.at[k, 3], (up, left)),
            (col_tx.at[k, 1, pl.ds(0, 1)], cor_rx.at[k, 2], (up, right)),
            (col_tx.at[k, 0, pl.ds(q - 1, 1)], cor_rx.at[k, 1], (down, left)),
            (col_tx.at[k, 1, pl.ds(q - 1, 1)], cor_rx.at[k, 0], (down, right)),
            (row_tx.at[k, 0], row_rx.at[k, 1], (up, me_s)),
            (row_tx.at[k, 1], row_rx.at[k, 0], (down, me_s)),
            (col_tx.at[k, 0], col_rx.at[k, 1], (me_c, left)),
            (col_tx.at[k, 1], col_rx.at[k, 0], (me_c, right)),
        ]
        return [
            pltpu.make_async_remote_copy(
                src_ref=src, dst_ref=dst, send_sem=htx_sem.at[k, e], recv_sem=hrx_sem.at[k, e],
                device_id=where, device_id_type=MESH)
            for e, (src, dst, where) in enumerate(plan)
        ]

    def send(k, tops):
        col_tx[k, 0], col_tx[k, 1] = tops
        for copy in halo_copies(k):
            copy.start()

    def arrive(k):
        for copy in halo_copies(k):
            copy.wait_recv()
        ph = lax.broadcasted_iota(jnp.int32, (1, LANES), 1) % 4
        edge_row = lax.broadcasted_iota(jnp.int32, (q, LANES), 0)
        merged = []
        for side in range(2):
            above, below = cor_rx[k, side], cor_rx[k, 2 + side]
            above = jnp.where(ph == 0, pltpu.roll(above, LANES - 3, 1), 0.0)
            below = jnp.where(ph == 3, pltpu.roll(below, 3, 1), 0.0)
            c = col_rx[k, side]
            c = c + jnp.where(edge_row == 0, above, 0.0) + jnp.where(edge_row == q - 1, below, 0.0)
            merged.append(c)
        return merged

    def assembled(k, m, slot, merged):
        t = load(w, m)
        t[0] = t[0] + jnp.where(row_at == 0, row_rx[k, 0, pl.ds(slot, 1), :], 0.0)
        t[3] = t[3] + jnp.where(row_at == q - 1, row_rx[k, 1, pl.ds(slot, 1), :], 0.0)
        out = []
        for p in range(4):
            at = 4 * slot + p
            c = t[p] + jnp.where(
                take_next, pltpu.roll(t[p], cols - 1, 1),
                jnp.where(take_prev, pltpu.roll(t[p], 1, 1), 0.0))
            a = jnp.where(lane == 0, pltpu.roll(merged[0], LANES - at, 1), 0.0)
            b = jnp.where(lane == LANES - 1, pltpu.roll(merged[1], LANES - 1 - at, 1), 0.0)
            pieces = [c[:, e * LANES:(e + 1) * LANES] for e in range(tiles)]
            pieces[0] = pieces[0] + a
            pieces[-1] = pieces[-1] + b
            out.append(jnp.concatenate(pieces, axis=1))
        return out

    edge_w, mid_w = f32(1.0 / 6.0), f32(5.0 / 6.0)
    col_w = jnp.where(on_edge, edge_w, mid_w)
    mw, fw = [], []
    for copy in loads:
        copy.wait()
    for p in range(4):
        grid_w = col_w * (edge_w if p in (0, 3) else mid_w)
        mw.append(strided([factors.at[0, c] for c in range(tiles)], p, q) * grid_w)
        fw.append(strided([factors.at[1, c] for c in range(tiles)], p, q) * grid_w)
        mass[p * q:(p + 1) * q, :] = mw[p]
        flux[p * q:(p + 1) * q, :] = fw[p]
    zero = jnp.zeros((q, LANES), f32)
    tops = pack(0, modes, per, mw, (zero, zero))
    div_load.wait()
    table = div_ref[:cols, :].astype(f32) + div_ref[2 * cols:, :].astype(f32)
    by_cols = jnp.dot(flux[...], table * table, precision=lax.Precision.HIGHEST,
                      preferred_element_type=f32)
    squared = SLOPES * SLOPES
    lap = [combo(squared[:, a], fw) + by_cols[a * q:(a + 1) * q, :] for a in range(4)]
    tops = pack(0, modes + 1, per + 1, lap, tops)
    for copy in sources:
        copy.wait()
    for g in range(groups):

        def start_body(slot, carry, g=g):
            m = g * per + slot
            h = [strided([source.at[c, m] for c in range(tiles)], p, q)
                 * mass[p * q:(p + 1) * q, :] for p in range(4)]
            return pack(g, m, slot, h, carry)

        tops = lax.fori_loop(0, per, start_body, tops if g == 0 else (zero, zero), unroll=UNROLL)
        if g == 0:
            pl.semaphore_wait(barrier, n - 1)
        send(g, tops)
    scale_load.wait()
    grad_load.wait()

    pad = (lax.broadcasted_iota(jnp.int32, (1, LANES), 1) >= per).astype(f32)
    eye = lax.broadcasted_iota(jnp.int32, (slots, LANES), 0) == lax.broadcasted_iota(
        jnp.int32, (slots, LANES), 1)

    def update(it, g, m, slot, ww):
        a, b = coef[g, 0, pl.ds(slot, 1), :], coef[g, 1, pl.ds(slot, 1), :]
        zz = load(z, m)
        if it > 1:
            dd, ss = load(d, m), load(s, m)
            zz = [u + b * v for u, v in zip(zz, dd)]
            ww = [u + b * v for u, v in zip(ww, ss)]
            xx = [u + a * v for u, v in zip(load(x, m), zz)]
        else:
            xx = [a * v for v in zz]
        rr = [u - a * v for u, v in zip(load(r, m), ww)]
        return zz, ww, xx, rr

    def fill(slot, parts):
        v = jnp.concatenate(parts, axis=0)
        top = v.astype(bf16)
        at = pl.ds(pl.multiple_of(slot * rows, rows), rows)
        zcat[at, :cols] = top
        zcat[at, cols:] = (v - top.astype(f32)).astype(bf16)

    def multiply(table_ref):
        gout[...] = (
            jnp.dot(zcat[...], table_ref[:2 * cols, :], preferred_element_type=f32)
            + jnp.dot(zcat[:, :cols], table_ref[2 * cols:, :], preferred_element_type=f32))

    old = [None] * groups

    def coefficients(it, g):
        k = it * groups + g
        gathered = ar_rx.at[k, pl.ds(1, n - 1)]
        pltpu.make_async_copy(gathered, gathered, arx_sem.at[k]).wait()
        total = jnp.sum(ar_rx[k], axis=0)
        rho, curve_sum = total[0:1] + pad, total[1:2] + pad
        if it == 0:
            mixing = jnp.zeros_like(rho)
            step_len = rho / curve_sum
        else:
            mixing = rho / old[g][0]
            step_len = rho / (curve_sum - mixing * rho / old[g][1])
        for e, line in enumerate((step_len, mixing)):
            tall = jnp.sum(jnp.where(eye, line, 0.0), axis=1, keepdims=True)
            coef[g, e] = jnp.broadcast_to(tall, (slots, cols))
        old[g] = (rho, step_len)

    for it in range(ITERS):
        for g in range(groups):
            base = g * per
            k = it * groups + g
            merged = arrive(k)
            if it == 0 and g == 0:
                for e in range(2):
                    save(w, modes + e, assembled(k, modes + e, per + e, merged))
            if it > 0:
                coefficients(it - 1, g)

            def first(slot, carry, it=it, g=g, k=k, base=base, merged=merged):
                m = base + slot
                ww = assembled(k, m, slot, merged)
                if it == 0:
                    rr = ww
                    inv = [1.0 / (u + scale_ref[m] * v)
                           for u, v in zip(load(w, modes), load(w, modes + 1))]
                    save(invp, m, inv)
                else:
                    dd, ss, xx, rr = update(it, g, m, slot, ww)
                    save(x, m, xx)
                    save(d, m, dd)
                    save(s, m, ss)
                    inv = load(invp, m)
                save(r, m, rr)
                zz = [u * v for u, v in zip(rr, inv)]
                save(z, m, zz)
                fill(slot, zz)
                rz = [u * v for u, v in zip(rr, zz)]
                rho = (rz[0] + rz[3]) * 0.5 + (rz[1] + rz[2])
                rho = jnp.where(on_edge, rho * 0.5, rho)
                sums[0, pl.ds(slot, 1), :] = jnp.sum(rho, axis=0, keepdims=True)
                f = load2(flux)
                fg = [f[a] * combo(SLOPES[a], zz) * scale_ref[m] for a in range(4)]
                ms = load2(mass)
                save(w, m, [ms[a] * zz[a] + combo(SLOPES[:, a], fg) for a in range(4)])
                return carry

            lax.fori_loop(0, per, first, 0, unroll=UNROLL)
            multiply(grad_ref)

            def second(slot, carry, base=base):
                grad = gout[pl.ds(pl.multiple_of(slot * rows, rows), rows), :]
                fill(slot, [flux[...] * grad * scale_ref[base + slot]])
                return carry

            lax.fori_loop(0, per, second, 0, unroll=UNROLL)
            multiply(div_ref)

            def third(slot, carry, k=k, base=base):
                m = base + slot
                zz = load(z, m)
                h = [u + gout[pl.ds(pl.multiple_of(slot * rows + p * q, q), q), :]
                     for p, u in enumerate(load(w, m))]
                zh = zz[0] * h[0] + zz[1] * h[1] + zz[2] * h[2] + zz[3] * h[3]
                sums[1, pl.ds(slot, 1), :] = jnp.sum(zh, axis=0, keepdims=True)
                return pack(k + groups, m, slot, h, carry)

            tops = lax.fori_loop(0, per, third, (zero, zero), unroll=UNROLL)
            send(k + groups, tops)
            for e in range(2):
                part = jnp.sum(sums[e], axis=1, keepdims=True)
                line = jnp.sum(jnp.where(eye, part, 0.0), axis=0, keepdims=True)
                ar_tx[k, e:e + 1, :] = line
                ar_rx[k, 0, e:e + 1, :] = line

            def spread(offset, carry, k=k):
                pltpu.make_async_remote_copy(
                    src_ref=ar_tx.at[k], dst_ref=ar_rx.at[k, offset],
                    send_sem=atx_sem.at[k], recv_sem=arx_sem.at[k],
                    device_id=place(offset), device_id_type=MESH).start()
                return carry

            lax.fori_loop(1, n, spread, 0)

    for g in range(groups):
        k = ITERS * groups + g
        merged = arrive(k)
        coefficients(ITERS - 1, g)

        def last(slot, carry, g=g, k=k, merged=merged):
            m = g * per + slot
            _, _, xx, rr = update(ITERS, g, m, slot, assembled(k, m, slot, merged))
            save(x, m, xx)
            save(r, m, rr)
            return carry

        lax.fori_loop(0, per, last, 0, unroll=UNROLL)

    for k in range((ITERS + 1) * groups):
        for copy in halo_copies(k):
            copy.wait_send()
    for k in range(ITERS * groups):
        sent = ar_rx.at[k, pl.ds(1, n - 1)]
        pltpu.make_async_copy(sent, sent, atx_sem.at[k]).wait()


def node_order(x, r, sol_ref, res_ref, sol_buf, res_buf, sem):
    modes, rows, cols = x.shape
    q, tiles = rows // 4, cols // LANES

    def stores(m):
        return [
            pltpu.make_async_copy(
                buf.at[c, m], out.at[m, :, pl.ds(c * LANES, LANES)], sem.at[k, c, m])
            for k, (buf, out) in enumerate(((sol_buf, sol_ref), (res_buf, res_ref)))
            for c in range(tiles)
        ]

    def body(m, carry):
        for c in range(tiles):
            for p in range(4):
                cut = slice(c * LANES, (c + 1) * LANES)
                sol_buf[c, m, pl.ds(p, q, stride=4), :] = x[m, p * q:(p + 1) * q, cut]
                res_buf[c, m, pl.ds(p, q, stride=4), :] = r[m, p * q:(p + 1) * q, cut]
        for copy in stores(m):
            copy.start()
        return carry

    lax.fori_loop(0, modes, body, 0)

    def drain(m, carry):
        for copy in stores(m):
            copy.wait()
        return carry

    lax.fori_loop(0, modes, drain, 0)


def strided(refs, p, q):
    return jnp.concatenate([ref[pl.ds(p, q, stride=4), :] for ref in refs], axis=1)


def stack_table(table):
    top = table.astype(bf16)
    low = (table - top.astype(np.float32)).astype(bf16)
    return np.concatenate([top, top, low], axis=0)


def shards(nc, ns, forcing, metric, jacobian, mode_scale):
    modes, rows, cols = forcing.shape
    block = np.kron(np.eye(cols // 4), SLOPES).astype(np.float32)
    grad, div = stack_table(block.T), stack_table(block)
    n, q, tiles = nc * ns, rows // 4, cols // LANES
    groups = GROUPS if modes % GROUPS == 0 else 1
    per = modes // groups
    slots = -(-(per + 2) // 8) * 8
    vm = pl.BlockSpec(memory_space=pltpu.VMEM)
    hbm = pl.BlockSpec(memory_space=pltpu.HBM)
    rounds, sums = (ITERS + 1) * groups, ITERS * groups
    field = pltpu.VMEM((modes, rows, cols), f32)
    split = pltpu.VMEM((tiles, modes, rows, LANES), f32)
    table = pltpu.VMEM(grad.shape, bf16)
    shape = jax.ShapeDtypeStruct(forcing.shape, f32)
    x, r = pl.pallas_call(
        functools.partial(kernel, nc, ns, modes, groups),
        out_shape=[shape] * 2,
        in_specs=[hbm] * 6,
        out_specs=[vm, vm],
        scratch_shapes=[
            field, field, field,
            pltpu.VMEM((modes + 2, rows, cols), f32),
            field,
            pltpu.VMEM((rows, cols), f32),
            pltpu.VMEM((rows, cols), f32),
            pltpu.VMEM((per * rows, 2 * cols), bf16),
            pltpu.VMEM((per * rows, cols), f32),
            pltpu.VMEM((2, slots, cols), f32),
            pltpu.VMEM((groups, 2, slots, cols), f32),
            pltpu.VMEM((rounds, 2, slots, cols), f32),
            pltpu.VMEM((rounds, 2, slots, cols), f32),
            pltpu.VMEM((rounds, 2, q, LANES), f32),
            pltpu.VMEM((rounds, 2, q, LANES), f32),
            pltpu.VMEM((rounds, 4, 1, LANES), f32),
            pltpu.VMEM((sums, 2, LANES), f32),
            pltpu.VMEM((sums, n, 2, LANES), f32),
            split,
            pltpu.VMEM((2, tiles, rows, LANES), f32),
            table, table,
            pltpu.SMEM((modes,), f32),
            pltpu.SemaphoreType.DMA((rounds, 8)),
            pltpu.SemaphoreType.DMA((rounds, 8)),
            pltpu.SemaphoreType.DMA((sums,)),
            pltpu.SemaphoreType.DMA((sums,)),
            pltpu.SemaphoreType.DMA((3, tiles)),
            pltpu.SemaphoreType.DMA((3,)),
        ],
        compiler_params=pltpu.CompilerParams(
            collective_id=0, has_side_effects=True, vmem_limit_bytes=41943040),
    )(*[pltpu.with_memory_space_constraint(v, pltpu.HBM) for v in (mode_scale, forcing, metric, jacobian, jnp.asarray(grad), jnp.asarray(div))])
    return pl.pallas_call(
        node_order,
        out_shape=[shape] * 2,
        in_specs=[vm, vm],
        out_specs=[hbm, hbm],
        scratch_shapes=[split, split, pltpu.SemaphoreType.DMA((2, tiles, modes))],
        compiler_params=pltpu.CompilerParams(vmem_limit_bytes=16 * 1024 * 1024),
    )(x, r)


def solution(mesh):
    placed = (P(None, "curve", "sub"), P("curve", "sub"), P("curve", "sub"), P())
    return jax.shard_map(
        functools.partial(shards, mesh.shape["curve"], mesh.shape["sub"]),
        mesh=mesh,
        in_specs=placed,
        out_specs=(P(None, "curve", "sub"), P(None, "curve", "sub")),
        check_vma=False,
    )
```

```python
import functools
import math

import jax
import jax.numpy as jnp
import numpy as np
from jax import lax
from jax.experimental import pallas as pl
from jax.experimental.pallas import tpu as pltpu
from jax.sharding import PartitionSpec as P

ITERS = 3
GROUPS = 2
UNROLL = True
MESH = pl.DeviceIdType.MESH
LANES = 128
f32 = jnp.float32
bf16 = jnp.bfloat16


def gll_tables():
    points = np.array([-1.0, -1.0 / math.sqrt(5.0), 1.0 / math.sqrt(5.0), 1.0])
    weights = np.array([1.0 / 6.0, 5.0 / 6.0, 5.0 / 6.0, 1.0 / 6.0])
    factor = np.array(
        [np.prod([points[j] - points[m] for m in range(4) if m != j]) for j in range(4)]
    )
    slopes = np.zeros((4, 4))
    for i in range(4):
        for j in range(4):
            if i != j:
                slopes[i, j] = factor[i] / (factor[j] * (points[i] - points[j]))
        slopes[i, i] = sum((1.0 / (points[i] - points[m]) for m in range(4) if m != i))
    return (slopes, weights)


SLOPES, WEIGHTS = gll_tables()


def combo(coefs, parts):
    total = None
    for c, v in zip(coefs, parts):
        if abs(c) < 1e-12:
            continue
        term = v * f32(c)
        total = term if total is None else total + term
    return total


def kernel(
    nc, ns, modes, groups,
    scale_hbm, forcing_ref, metric_ref, jac_ref, grad_hbm, div_hbm,
    x, r,
    z, d, s, w, invp, mass, flux, zcat, gout, sums, coef,
    row_tx, row_rx, col_tx, col_rx, cor_rx, ar_tx, ar_rx,
    source, factors, grad_ref, div_ref, scale_ref,
    htx_sem, hrx_sem, atx_sem, arx_sem, in_sem, table_sem,
):
    rows, cols = metric_ref.shape
    q = rows // 4
    n = nc * ns
    half = cols - LANES
    tiles = cols // LANES
    per = modes // groups
    slots = row_tx.shape[2]
    loads, sources = [], []
    for c in range(tiles):
        cut = pl.ds(c * LANES, LANES)
        loads += [
            pltpu.make_async_copy(jac_ref.at[:, cut], factors.at[0, c], in_sem.at[0, c]),
            pltpu.make_async_copy(metric_ref.at[:, cut], factors.at[1, c], in_sem.at[1, c]),
        ]
        sources.append(
            pltpu.make_async_copy(forcing_ref.at[:, :, cut], source.at[c], in_sem.at[2, c]))
    div_load = pltpu.make_async_copy(div_hbm, div_ref, table_sem.at[0])
    grad_load = pltpu.make_async_copy(grad_hbm, grad_ref, table_sem.at[1])
    scale_load = pltpu.make_async_copy(scale_hbm, scale_ref, table_sem.at[2])
    for copy in loads + sources + [div_load, scale_load, grad_load]:
        copy.start()

    me_c, me_s = lax.axis_index("curve"), lax.axis_index("sub")
    me = me_c * ns + me_s
    up, down = lax.rem(me_c + nc - 1, nc), lax.rem(me_c + 1, nc)
    left, right = lax.rem(me_s + ns - 1, ns), lax.rem(me_s + 1, ns)

    def place(offset):
        target = lax.rem(me + offset, n)
        return (target // ns, lax.rem(target, ns))

    barrier = pltpu.get_barrier_semaphore()

    def greet(offset, carry):
        pl.semaphore_signal(barrier, inc=1, device_id=place(offset), device_id_type=MESH)
        return carry

    lax.fori_loop(1, n, greet, 0)

    lane_full = lax.broadcasted_iota(jnp.int32, (q, cols), 1)
    lane = lax.broadcasted_iota(jnp.int32, (q, LANES), 1)
    row_at = lax.broadcasted_iota(jnp.int32, (q, cols), 0)
    phase = lane_full % 4
    on_edge = (phase == 0) | (phase == 3)
    take_next = (phase == 3) & (lane_full != cols - 1)
    take_prev = (phase == 0) & (lane_full != 0)

    def load(ref, m):
        return [ref[m, p * q:(p + 1) * q, :] for p in range(4)]

    def save(ref, m, parts):
        for p in range(4):
            ref[m, p * q:(p + 1) * q, :] = parts[p]

    def load2(ref):
        return [ref[p * q:(p + 1) * q, :] for p in range(4)]

    def pack(k, m, slot, h, tops):
        lo, hi = tops
        row_tx[k, 0, pl.ds(slot, 1), :] = h[0][0:1, :]
        row_tx[k, 1, pl.ds(slot, 1), :] = h[3][q - 1:q, :]
        t0 = h[0] + jnp.where(row_at == 0, 0.0, pltpu.roll(h[3], 1, 0))
        t3 = h[3] + jnp.where(row_at == q - 1, 0.0, pltpu.roll(h[0], q - 1, 0))
        t = [t0, h[1], h[2], t3]
        save(w, m, t)
        for p in range(4):
            at = 4 * slot + p
            lo = jnp.where(lane == at, pltpu.roll(t[p][:, :LANES], at, 1), lo)
            hi = jnp.where(lane == at, pltpu.roll(t[p][:, half:], at + 1, 1), hi)
        return lo, hi

    def halo_copies(k):
        plan = [
            (row_tx.at[k, 0], row_rx.at[k, 1], (up, me_s)),
            (row_tx.at[k, 1], row_rx.at[k, 0], (down, me_s)),
            (col_tx.at[k, 0, pl.ds(0, 1)], cor_rx.at[k, 3], (up, left)),
            (col_tx.at[k, 1, pl.ds(0, 1)], cor_rx.at[k, 2], (up, right)),
            (col_tx.at[k, 0, pl.ds(q - 1, 1)], cor_rx.at[k, 1], (down, left)),
            (col_tx.at[k, 1, pl.ds(q - 1, 1)], cor_rx.at[k, 0], (down, right)),
            (col_tx.at[k, 0], col_rx.at[k, 1], (me_c, left)),
            (col_tx.at[k, 1], col_rx.at[k, 0], (me_c, right)),
        ]
        return [
            pltpu.make_async_remote_copy(
                src_ref=src, dst_ref=dst, send_sem=htx_sem.at[k, e], recv_sem=hrx_sem.at[k, e],
                device_id=where, device_id_type=MESH)
            for e, (src, dst, where) in enumerate(plan)
        ]

    def send(k, tops):
        col_tx[k, 0], col_tx[k, 1] = tops
        for copy in halo_copies(k):
            copy.start()

    def arrive(k):
        for copy in halo_copies(k):
            copy.wait_recv()
        ph = lax.broadcasted_iota(jnp.int32, (1, LANES), 1) % 4
        edge_row = lax.broadcasted_iota(jnp.int32, (q, LANES), 0)
        merged = []
        for side in range(2):
            above, below = cor_rx[k, side], cor_rx[k, 2 + side]
            above = jnp.where(ph == 0, pltpu.roll(above, LANES - 3, 1), 0.0)
            below = jnp.where(ph == 3, pltpu.roll(below, 3, 1), 0.0)
            c = col_rx[k, side]
            c = c + jnp.where(edge_row == 0, above, 0.0) + jnp.where(edge_row == q - 1, below, 0.0)
            merged.append(c)
        return merged

    def assembled(k, m, slot, merged):
        t = load(w, m)
        t[0] = t[0] + jnp.where(row_at == 0, row_rx[k, 0, pl.ds(slot, 1), :], 0.0)
        t[3] = t[3] + jnp.where(row_at == q - 1, row_rx[k, 1, pl.ds(slot, 1), :], 0.0)
        out = []
        for p in range(4):
            at = 4 * slot + p
            c = t[p] + jnp.where(
                take_next, pltpu.roll(t[p], cols - 1, 1),
                jnp.where(take_prev, pltpu.roll(t[p], 1, 1), 0.0))
            a = jnp.where(lane == 0, pltpu.roll(merged[0], LANES - at, 1), 0.0)
            b = jnp.where(lane == LANES - 1, pltpu.roll(merged[1], LANES - 1 - at, 1), 0.0)
            pieces = [c[:, e * LANES:(e + 1) * LANES] for e in range(tiles)]
            pieces[0] = pieces[0] + a
            pieces[-1] = pieces[-1] + b
            out.append(jnp.concatenate(pieces, axis=1))
        return out

    edge_w, mid_w = f32(1.0 / 6.0), f32(5.0 / 6.0)
    col_w = jnp.where(on_edge, edge_w, mid_w)
    mw, fw = [], []
    for copy in loads:
        copy.wait()
    for p in range(4):
        grid_w = col_w * (edge_w if p in (0, 3) else mid_w)
        mw.append(strided([factors.at[0, c] for c in range(tiles)], p, q) * grid_w)
        fw.append(strided([factors.at[1, c] for c in range(tiles)], p, q) * grid_w)
        mass[p * q:(p + 1) * q, :] = mw[p]
        flux[p * q:(p + 1) * q, :] = fw[p]
    zero = jnp.zeros((q, LANES), f32)
    tops = pack(0, modes, per, mw, (zero, zero))
    div_load.wait()
    table = div_ref[:cols, :].astype(f32) + div_ref[2 * cols:, :].astype(f32)
    by_cols = jnp.dot(flux[...], table * table, precision=lax.Precision.HIGHEST,
                      preferred_element_type=f32)
    squared = SLOPES * SLOPES
    lap = [combo(squared[:, a], fw) + by_cols[a * q:(a + 1) * q, :] for a in range(4)]
    tops = pack(0, modes + 1, per + 1, lap, tops)
    for copy in sources:
        copy.wait()
    for g in range(groups):

        def start_body(slot, carry, g=g):
            m = g * per + slot
            h = [strided([source.at[c, m] for c in range(tiles)], p, q)
                 * mass[p * q:(p + 1) * q, :] for p in range(4)]
            return pack(g, m, slot, h, carry)

        tops = lax.fori_loop(0, per, start_body, tops if g == 0 else (zero, zero), unroll=UNROLL)
        if g == 0:
            pl.semaphore_wait(barrier, n - 1)
        send(g, tops)
    scale_load.wait()
    grad_load.wait()

    pad = (lax.broadcasted_iota(jnp.int32, (1, LANES), 1) >= per).astype(f32)
    eye = lax.broadcasted_iota(jnp.int32, (slots, LANES), 0) == lax.broadcasted_iota(
        jnp.int32, (slots, LANES), 1)

    def update(it, g, m, slot, ww):
        a, b = coef[g, 0, pl.ds(slot, 1), :], coef[g, 1, pl.ds(slot, 1), :]
        zz = load(z, m)
        if it > 1:
            dd, ss = load(d, m), load(s, m)
            zz = [u + b * v for u, v in zip(zz, dd)]
            ww = [u + b * v for u, v in zip(ww, ss)]
            xx = [u + a * v for u, v in zip(load(x, m), zz)]
        else:
            xx = [a * v for v in zz]
        rr = [u - a * v for u, v in zip(load(r, m), ww)]
        return zz, ww, xx, rr

    def fill(slot, parts):
        v = jnp.concatenate(parts, axis=0)
        top = v.astype(bf16)
        at = pl.ds(pl.multiple_of(slot * rows, rows), rows)
        zcat[at, :cols] = top
        zcat[at, cols:] = (v - top.astype(f32)).astype(bf16)

    def multiply(table_ref):
        gout[...] = (
            jnp.dot(zcat[...], table_ref[:2 * cols, :], preferred_element_type=f32)
            + jnp.dot(zcat[:, :cols], table_ref[2 * cols:, :], preferred_element_type=f32))

    old = [None] * groups

    def coefficients(it, g):
        k = it * groups + g
        gathered = ar_rx.at[k, pl.ds(1, n - 1)]
        pltpu.make_async_copy(gathered, gathered, arx_sem.at[k]).wait()
        total = jnp.sum(ar_rx[k], axis=0)
        rho, curve_sum = total[0:1] + pad, total[1:2] + pad
        if it == 0:
            mixing = jnp.zeros_like(rho)
            step_len = rho / curve_sum
        else:
            mixing = rho / old[g][0]
            step_len = rho / (curve_sum - mixing * rho / old[g][1])
        for e, line in enumerate((step_len, mixing)):
            tall = jnp.sum(jnp.where(eye, line, 0.0), axis=1, keepdims=True)
            coef[g, e] = jnp.broadcast_to(tall, (slots, cols))
        old[g] = (rho, step_len)

    for it in range(ITERS):
        for g in range(groups):
            base = g * per
            k = it * groups + g
            merged = arrive(k)
            if it == 0 and g == 0:
                for e in range(2):
                    save(w, modes + e, assembled(k, modes + e, per + e, merged))
            if it > 0:
                coefficients(it - 1, g)

            def first(slot, carry, it=it, g=g, k=k, base=base, merged=merged):
                m = base + slot
                ww = assembled(k, m, slot, merged)
                if it == 0:
                    rr = ww
                    inv = [1.0 / (u + scale_ref[m] * v)
                           for u, v in zip(load(w, modes), load(w, modes + 1))]
                    save(invp, m, inv)
                else:
                    dd, ss, xx, rr = update(it, g, m, slot, ww)
                    save(x, m, xx)
                    save(d, m, dd)
                    save(s, m, ss)
                    inv = load(invp, m)
                save(r, m, rr)
                zz = [u * v for u, v in zip(rr, inv)]
                save(z, m, zz)
                fill(slot, zz)
                rz = [u * v for u, v in zip(rr, zz)]
                rho = (rz[0] + rz[3]) * 0.5 + (rz[1] + rz[2])
                rho = jnp.where(on_edge, rho * 0.5, rho)
                sums[0, pl.ds(slot, 1), :] = jnp.sum(rho, axis=0, keepdims=True)
                f = load2(flux)
                fg = [f[a] * combo(SLOPES[a], zz) * scale_ref[m] for a in range(4)]
                ms = load2(mass)
                save(w, m, [ms[a] * zz[a] + combo(SLOPES[:, a], fg) for a in range(4)])
                return carry

            lax.fori_loop(0, per, first, 0, unroll=UNROLL)
            multiply(grad_ref)

            def second(slot, carry, base=base):
                grad = gout[pl.ds(pl.multiple_of(slot * rows, rows), rows), :]
                fill(slot, [flux[...] * grad * scale_ref[base + slot]])
                return carry

            lax.fori_loop(0, per, second, 0, unroll=UNROLL)
            multiply(div_ref)

            def third(slot, carry, k=k, base=base):
                m = base + slot
                zz = load(z, m)
                h = [u + gout[pl.ds(pl.multiple_of(slot * rows + p * q, q), q), :]
                     for p, u in enumerate(load(w, m))]
                zh = zz[0] * h[0] + zz[1] * h[1] + zz[2] * h[2] + zz[3] * h[3]
                sums[1, pl.ds(slot, 1), :] = jnp.sum(zh, axis=0, keepdims=True)
                return pack(k + groups, m, slot, h, carry)

            tops = lax.fori_loop(0, per, third, (zero, zero), unroll=UNROLL)
            send(k + groups, tops)
            for e in range(2):
                part = jnp.sum(sums[e], axis=1, keepdims=True)
                line = jnp.sum(jnp.where(eye, part, 0.0), axis=0, keepdims=True)
                ar_tx[k, e:e + 1, :] = line
                ar_rx[k, 0, e:e + 1, :] = line

            def spread(offset, carry, k=k):
                pltpu.make_async_remote_copy(
                    src_ref=ar_tx.at[k], dst_ref=ar_rx.at[k, offset],
                    send_sem=atx_sem.at[k], recv_sem=arx_sem.at[k],
                    device_id=place(offset), device_id_type=MESH).start()
                return carry

            lax.fori_loop(1, n, spread, 0, unroll=True if n <= 32 else 1)

    for g in range(groups):
        k = ITERS * groups + g
        merged = arrive(k)
        coefficients(ITERS - 1, g)

        def last(slot, carry, g=g, k=k, merged=merged):
            m = g * per + slot
            _, _, xx, rr = update(ITERS, g, m, slot, assembled(k, m, slot, merged))
            save(x, m, xx)
            save(r, m, rr)
            return carry

        lax.fori_loop(0, per, last, 0, unroll=UNROLL)

    for k in range((ITERS + 1) * groups):
        for copy in halo_copies(k):
            copy.wait_send()
    for k in range(ITERS * groups):
        sent = ar_rx.at[k, pl.ds(1, n - 1)]
        pltpu.make_async_copy(sent, sent, atx_sem.at[k]).wait()


def node_order(x, r, sol_ref, res_ref, sol_buf, res_buf, sem):
    modes, rows, cols = x.shape
    q, tiles = rows // 4, cols // LANES

    def stores(m):
        return [
            pltpu.make_async_copy(
                buf.at[c, m], out.at[m, :, pl.ds(c * LANES, LANES)], sem.at[k, c, m])
            for k, (buf, out) in enumerate(((sol_buf, sol_ref), (res_buf, res_ref)))
            for c in range(tiles)
        ]

    def body(m, carry):
        for c in range(tiles):
            for p in range(4):
                cut = slice(c * LANES, (c + 1) * LANES)
                sol_buf[c, m, pl.ds(p, q, stride=4), :] = x[m, p * q:(p + 1) * q, cut]
                res_buf[c, m, pl.ds(p, q, stride=4), :] = r[m, p * q:(p + 1) * q, cut]
        for copy in stores(m):
            copy.start()
        return carry

    lax.fori_loop(0, modes, body, 0)

    def drain(m, carry):
        for copy in stores(m):
            copy.wait()
        return carry

    lax.fori_loop(0, modes, drain, 0)


def strided(refs, p, q):
    return jnp.concatenate([ref[pl.ds(p, q, stride=4), :] for ref in refs], axis=1)


def stack_table(table):
    top = table.astype(bf16)
    low = (table - top.astype(np.float32)).astype(bf16)
    return np.concatenate([top, top, low], axis=0)


def shards(nc, ns, forcing, metric, jacobian, mode_scale):
    modes, rows, cols = forcing.shape
    block = np.kron(np.eye(cols // 4), SLOPES).astype(np.float32)
    grad, div = stack_table(block.T), stack_table(block)
    n, q, tiles = nc * ns, rows // 4, cols // LANES
    groups = GROUPS if modes % GROUPS == 0 else 1
    per = modes // groups
    slots = -(-(per + 2) // 8) * 8
    vm = pl.BlockSpec(memory_space=pltpu.VMEM)
    hbm = pl.BlockSpec(memory_space=pltpu.HBM)
    rounds, sums = (ITERS + 1) * groups, ITERS * groups
    field = pltpu.VMEM((modes, rows, cols), f32)
    split = pltpu.VMEM((tiles, modes, rows, LANES), f32)
    table = pltpu.VMEM(grad.shape, bf16)
    shape = jax.ShapeDtypeStruct(forcing.shape, f32)
    x, r = pl.pallas_call(
        functools.partial(kernel, nc, ns, modes, groups),
        out_shape=[shape] * 2,
        in_specs=[hbm] * 6,
        out_specs=[vm, vm],
        scratch_shapes=[
            field, field, field,
            pltpu.VMEM((modes + 2, rows, cols), f32),
            field,
            pltpu.VMEM((rows, cols), f32),
            pltpu.VMEM((rows, cols), f32),
            pltpu.VMEM((per * rows, 2 * cols), bf16),
            pltpu.VMEM((per * rows, cols), f32),
            pltpu.VMEM((2, slots, cols), f32),
            pltpu.VMEM((groups, 2, slots, cols), f32),
            pltpu.VMEM((rounds, 2, slots, cols), f32),
            pltpu.VMEM((rounds, 2, slots, cols), f32),
            pltpu.VMEM((rounds, 2, q, LANES), f32),
            pltpu.VMEM((rounds, 2, q, LANES), f32),
            pltpu.VMEM((rounds, 4, 1, LANES), f32),
            pltpu.VMEM((sums, 2, LANES), f32),
            pltpu.VMEM((sums, n, 2, LANES), f32),
            split,
            pltpu.VMEM((2, tiles, rows, LANES), f32),
            table, table,
            pltpu.SMEM((modes,), f32),
            pltpu.SemaphoreType.DMA((rounds, 8)),
            pltpu.SemaphoreType.DMA((rounds, 8)),
            pltpu.SemaphoreType.DMA((sums,)),
            pltpu.SemaphoreType.DMA((sums,)),
            pltpu.SemaphoreType.DMA((3, tiles)),
            pltpu.SemaphoreType.DMA((3,)),
        ],
        compiler_params=pltpu.CompilerParams(
            collective_id=0, has_side_effects=True, vmem_limit_bytes=41943040),
    )(*[pltpu.with_memory_space_constraint(v, pltpu.HBM) for v in (mode_scale, forcing, metric, jacobian, jnp.asarray(grad), jnp.asarray(div))])
    return pl.pallas_call(
        node_order,
        out_shape=[shape] * 2,
        in_specs=[vm, vm],
        out_specs=[hbm, hbm],
        scratch_shapes=[split, split, pltpu.SemaphoreType.DMA((2, tiles, modes))],
        compiler_params=pltpu.CompilerParams(vmem_limit_bytes=16 * 1024 * 1024),
    )(x, r)


def solution(mesh):
    placed = (P(None, "curve", "sub"), P("curve", "sub"), P("curve", "sub"), P())
    return jax.shard_map(
        functools.partial(shards, mesh.shape["curve"], mesh.shape["sub"]),
        mesh=mesh,
        in_specs=placed,
        out_specs=(P(None, "curve", "sub"), P(None, "curve", "sub")),
        check_vma=False,
    )
```
